32 devices in a mesh: face: 8 (over z, y), col: 4 (over x, core).
Axes of the slice: x: 2, y: 2, z: 4, core: 2. Of those that a mesh axis runs over, the one named last changes fastest.
Arguments:
- fields: float32 [4, 160, 80, 128], P(None, 'face', 'col'), may hold values from -6 to 6
- metric_diag: float32 [2, 160, 80], P(None, 'face', 'col'), may hold values from 0.05 to 0.5
- metric_cross: float32 [160, 80], P('face', 'col'), may hold values from -0.1 to 0.1
- point_mass: float32 [160, 80], P('face', 'col'), may hold values from 0.5 to 2
Outputs:
- biharmonic: float32 [4, 160, 80, 128], P(None, 'face', 'col')
The draws below stay inside these ranges and needn't reach their ends.
All inputs are finite; a program needn't handle non-finite values.
Results may differ from the reference program's by a relative error of at most 0.00024.
Values sent between devices are 32-bit elements; how exact they have to be, the bound alone decides.
No kernel may reach another device: no remote copies, remote signals or barrier semaphores. Data moves between devices by JAX's collectives and lax.ppermute only.
A program may use at most 64 MiB of HBM per device.

```python
import math
import jax
import jax.numpy as jnp
import numpy as np
from jax import lax

FIELDS = 4
LEV = 128
NXP = 160
NYP = 80


def block_levels(key, shape, split, low, top_value):
    loudness = 1.0
    for axis_at, blocks in split:
        steps = jax.random.uniform(jax.random.fold_in(jax.random.fold_in(key, 6), axis_at), (blocks,), jnp.float32, low / len(split), top_value / len(split))
        loudness = loudness * jnp.repeat(jnp.exp(steps), shape[axis_at] // blocks).reshape((-1,) + (1,) * (len(shape) - 1 - axis_at))
    return loudness


def noise(own_key, shape, scale, bound, pieces=(), held_as=jnp.bfloat16):
    factor_of = block_levels(own_key, shape, pieces, -0.22, 0.18) if pieces else 1.0
    result = jax.random.normal(own_key, shape, jnp.float32) * scale * factor_of
    return jnp.minimum(jnp.maximum(result, -bound), bound).astype(held_as)


def setup_inputs(seed: int = 0) -> dict:
    key_list = jax.random.split(jax.random.key(seed), 5)
    fields = noise(key_list[0], (FIELDS, NXP, NYP, LEV), 1.0, 6.0, ((1, 8), (2, 4)), jnp.float32)
    metric_diag = jnp.clip(jnp.exp(math.log(0.5) - 2.3025851 * jax.random.uniform(key_list[1], (2, NXP, NYP), jnp.float32) ** block_levels(key_list[1], (2, NXP, NYP), ((1, 8), (2, 4)), -0.2, 0.2)), 0.05, 0.5)
    metric_cross = jnp.clip(jax.random.uniform(key_list[2], (NXP, NYP), jnp.float32, -0.1, 0.1) * block_levels(key_list[2], (NXP, NYP), ((0, 8), (1, 4)), -0.4, 0.0), -0.1, 0.1)
    point_mass = jnp.clip(jnp.exp(math.log(2.0) - 1.3862944 * jax.random.uniform(key_list[3], (NXP, NYP), jnp.float32) ** block_levels(key_list[3], (NXP, NYP), ((0, 8), (1, 4)), -0.2, 0.2)), 0.5, 2.0)
    return dict(fields=fields, metric_diag=metric_diag, metric_cross=metric_cross, point_mass=point_mass)


def derivative_table():
    small = 1.0 / np.sqrt(5.0)
    nodes = np.array([-1.0, -small, small, 1.0])
    count = nodes.shape[0]
    weights = np.array([np.prod([nodes[a] - nodes[k] for k in range(count) if k != a]) for a in range(count)])
    table = np.zeros((count, count))
    for a in range(count):
        for b in range(count):
            if a == b:
                table[a, b] = np.sum([1.0 / (nodes[a] - nodes[k]) for k in range(count) if k != a])
            else:
                table[a, b] = weights[a] / weights[b] / (nodes[a] - nodes[b])
    return jnp.asarray(table, jnp.float32)

def laplace(values, metric_diag, metric_cross):
    table = derivative_table()
    nfield, rows, cols, nlev = values.shape
    blocks_x = rows // 4
    blocks_y = cols // 4
    shaped = values.reshape(nfield, blocks_x, 4, blocks_y, 4, nlev)
    first_diag = metric_diag[0].reshape(1, blocks_x, 4, blocks_y, 4, 1)
    second_diag = metric_diag[1].reshape(1, blocks_x, 4, blocks_y, 4, 1)
    cross_term = metric_cross.reshape(1, blocks_x, 4, blocks_y, 4, 1)
    high = lax.Precision.HIGHEST
    grad_x = jnp.einsum('ab,febgcl->feagcl', table, shaped, precision=high)
    grad_y = jnp.einsum('cd,febgdl->febgcl', table, shaped, precision=high)
    flux_x = first_diag * grad_x + cross_term * grad_y
    flux_y = cross_term * grad_x + second_diag * grad_y
    weak = jnp.einsum('ba,febgcl->feagcl', table, flux_x, precision=high)
    weak = weak + jnp.einsum('dc,febgdl->febgcl', table, flux_y, precision=high)
    return (-weak).reshape(nfield, rows, cols, nlev)

def assemble(padded):
    rows = padded.shape[1] - 2
    cols = padded.shape[2] - 2
    row_local = jnp.arange(rows, dtype=jnp.int32) % 4
    col_local = jnp.arange(cols, dtype=jnp.int32) % 4
    row_low = (row_local == 0).astype(jnp.float32).reshape(1, rows, 1, 1)
    row_high = (row_local == 3).astype(jnp.float32).reshape(1, rows, 1, 1)
    col_low = (col_local == 0).astype(jnp.float32).reshape(1, 1, cols, 1)
    col_high = (col_local == 3).astype(jnp.float32).reshape(1, 1, cols, 1)
    summed = padded[:, 1:-1] + row_low * padded[:, :-2] + row_high * padded[:, 2:]
    return summed[:, :, 1:-1] + col_low * summed[:, :, :-2] + col_high * summed[:, :, 2:]

def wrap_pad(values):
    return jnp.pad(values, ((0, 0), (1, 1), (1, 1), (0, 0)), mode='wrap')

def reference(fields, metric_diag, metric_cross, point_mass):
    mass_sum = assemble(wrap_pad(point_mass[None, :, :, None]))
    first = assemble(wrap_pad(laplace(fields, metric_diag, metric_cross))) / mass_sum
    return assemble(wrap_pad(laplace(first, metric_diag, metric_cross))) / mass_sum
```

```python
import functools

import jax
import jax.numpy as jnp
import numpy as np
from jax import lax
from jax.experimental import pallas as pl
from jax.experimental.pallas import tpu as pltpu
from jax.sharding import PartitionSpec as P

F32 = jnp.float32
VMEM = pltpu.VMEM


def derivative_table():
    small = 1.0 / np.sqrt(5.0)
    nodes = np.array([-1.0, -small, small, 1.0])
    count = nodes.shape[0]
    weights = np.array(
        [np.prod([nodes[a] - nodes[k] for k in range(count) if k != a]) for a in range(count)]
    )
    table = np.zeros((count, count))
    for a in range(count):
        for b in range(count):
            if a == b:
                table[a, b] = np.sum([1.0 / (nodes[a] - nodes[k]) for k in range(count) if k != a])
            else:
                table[a, b] = weights[a] / weights[b] / (nodes[a] - nodes[b])
    return table.astype(np.float32)


D = derivative_table()


def upper_half():
    return lax.broadcasted_iota(jnp.int32, (8, 128), 0) >= 4


def swap(v):
    return pltpu.roll(v, 4, 0)


def col_coefs(table, upper):
    def vec(low, high):
        return jnp.where(upper, float(high), float(low)).astype(F32)

    return [
        [
            (vec(table[2 * h, 2 * k], table[2 * h + 1, 2 * k + 1]),
             vec(table[2 * h, 2 * k + 1], table[2 * h + 1, 2 * k]))
            for k in range(2)
        ]
        for h in range(2)
    ]


def col_apply(coefs, pair):
    swapped = [swap(v) for v in pair]
    out = []
    for h in range(2):
        (s0, x0), (s1, x1) = coefs[h]
        out.append((s0 * pair[0] + x0 * swapped[0]) + (s1 * pair[1] + x1 * swapped[1]))
    return out


def row_apply(table, vs):
    out = []
    for a in range(4):
        terms = [float(table[a, b]) * vs[b] for b in range(4)]
        out.append((terms[0] + terms[1]) + (terms[2] + terms[3]))
    return out


def spread(ref, row, pair, upper):
    line = jnp.broadcast_to(ref[pl.ds(row, 1), :], (8, 128))
    index = jnp.where(upper, 2 * pair + 1, 2 * pair).astype(jnp.int32)
    return jnp.take_along_axis(line, index, axis=1, mode="promise_in_bounds")


def laplace_band(load, e, pairs, mets, out_ref, colf_ref, coll_ref):
    d0, d1, dx = mets
    upper = upper_half()
    lower = jnp.logical_not(upper)
    fwd = col_coefs(D, upper)
    bwd = col_coefs(-D.T, upper)
    base = 4 * e
    done = [[None] * pairs for _ in range(4)]
    for g in range(pairs // 2):
        u = [[load(base + a, a, 2 * g + h) for h in range(2)] for a in range(4)]
        gx = [row_apply(D, [u[b][h] for b in range(4)]) for h in range(2)]
        fx = [[None] * 2 for _ in range(4)]
        wy = [None] * 4
        for a in range(4):
            gy = col_apply(fwd, u[a])
            fy = [None] * 2
            for h in range(2):
                cross = spread(dx, base + a, 2 * g + h, upper)
                fx[a][h] = spread(d0, base + a, 2 * g + h, upper) * gx[h][a] + cross * gy[h]
                fy[h] = cross * gx[h][a] + spread(d1, base + a, 2 * g + h, upper) * gy[h]
            wy[a] = col_apply(bwd, fy)
        for h in range(2):
            wx = row_apply(-D.T, [fx[b][h] for b in range(4)])
            for a in range(4):
                done[a][2 * g + h] = wx[a] + wy[a][h]
        if g > 0:
            for a in range(4):
                left, right = done[a][2 * g - 1], done[a][2 * g]
                done[a][2 * g - 1] = left + jnp.where(upper, swap(right), 0.0)
                done[a][2 * g] = right + jnp.where(lower, swap(left), 0.0)
        ready = []
        if g > 0:
            ready.append(2 * g - 1)
        ready.append(2 * g)
        if g == pairs // 2 - 1:
            ready.append(2 * g + 1)
        for p in ready:
            for a in range(4):
                out_ref[base + a, p] = done[a][p]

    @pl.when(e > 0)
    def _():
        for p in range(pairs):
            total = out_ref[base - 1, p] + out_ref[base, p]
            out_ref[base - 1, p] = total
            out_ref[base, p] = total


def col_edges(out_ref, rows, pairs, colf_ref, coll_ref):
    for r in range(rows):
        colf_ref[r] = out_ref[r, 0][0:4]
        coll_ref[r] = out_ref[r, pairs - 1][4:8]


def stage_metrics(md_ref, mc_ref, s0, s1, sx):
    cols = mc_ref.shape[1]
    s0[:, 0:cols] = md_ref[:, 0, :]
    s1[:, 0:cols] = md_ref[:, 1, :]
    sx[:, 0:cols] = mc_ref[...]


def first_kernel(u_ref, md_ref, mc_ref, mass_ref, out_ref, colf_ref, coll_ref, s0, s1, sx, sm):
    rows, pairs = u_ref.shape[:2]
    cols = 2 * pairs
    stage_metrics(md_ref, mc_ref, s0, s1, sx)
    sm[...] = jnp.ones_like(sm)
    sm[:, 0:cols] = mass_ref[...]

    def band(e, carry):
        laplace_band(
            lambda row, a, p: u_ref[row, p], e, pairs, (s0, s1, sx), out_ref, colf_ref, coll_ref
        )
        return carry

    lax.fori_loop(0, rows // 4, band, 0)
    col_edges(out_ref, rows, pairs, colf_ref, coll_ref)
    for q in range(rows // 4):
        part = sm[pl.ds(4 * q, 4), :]
        colf_ref[rows + q] = part
        coll_ref[rows + q] = part


def low_only(v):
    return jnp.concatenate([v, jnp.zeros_like(v)], axis=0)


def high_only(v):
    return jnp.concatenate([jnp.zeros_like(v), v], axis=0)


def row_edges(a_first, a_last, before, after, rowf_ref, rowl_ref, rows, pairs):
    for source, dest, row in ((a_first, rowf_ref, 0), (a_last, rowl_ref, rows - 1)):
        for p in range(pairs):
            v = source[0, p]
            if p == 0:
                v = v + low_only(before[row])
            if p == pairs - 1:
                v = v + high_only(after[row])
            dest[p] = v


def edge_kernel_mass(af, al, before, after, mass_ref, rowf_ref, rowl_ref, mcol_ref, sb, sa, sm):
    rows, cols = mass_ref.shape
    pairs = cols // 2
    row_edges(af, al, before, after, rowf_ref, rowl_ref, rows, pairs)
    for q in range(rows // 4):
        sb[pl.ds(4 * q, 4), :] = before[rows + q]
        sa[pl.ds(4 * q, 4), :] = after[rows + q]
    sm[...] = jnp.ones_like(sm)
    sm[pl.ds(0, rows), 0:cols] = mass_ref[...]
    m = sm[...]
    lane = lax.broadcasted_iota(jnp.int32, m.shape, 1)
    prev = jnp.where(lane == 0, pltpu.roll(sb[...], 128 - (cols - 1), 1), pltpu.roll(m, 1, 1))
    following = jnp.where(
        lane == cols - 1, pltpu.roll(sa[...], cols - 1, 1), pltpu.roll(m, 127, 1)
    )
    m = m + jnp.where(lane % 4 == 0, prev, 0.0) + jnp.where(lane % 4 == 3, following, 0.0)
    sm[...] = m
    mcol_ref[...] = sm[pl.ds(0, rows), :]
    rowf_ref[pairs] = jnp.broadcast_to(sm[pl.ds(0, 1), :], (8, 128))
    rowl_ref[pairs] = jnp.broadcast_to(sm[pl.ds(rows - 1, 1), :], (8, 128))


def edge_kernel(af, al, before, after, rowf_ref, rowl_ref, *, rows, pairs):
    row_edges(af, al, before, after, rowf_ref, rowl_ref, rows, pairs)


def whole_point(a_ref, rb, ra, before, after, row, a, p, e, last, pairs):
    v = a_ref[row, p]
    if a == 0:
        v = v + jnp.where(e == 0, rb[p], 0.0)
    if a == 3:
        v = v + jnp.where(e == last, ra[p], 0.0)
    if p == 0:
        v = v + low_only(before[row])
    if p == pairs - 1:
        v = v + high_only(after[row])
    return v


def second_kernel(
    a_ref, before, after, rb, ra, mcol_ref, md_ref, mc_ref,
    out_ref, colf_ref, coll_ref, inv_ref, s0, s1, sx,
):
    rows, pairs = a_ref.shape[:2]
    last = rows // 4 - 1
    stage_metrics(md_ref, mc_ref, s0, s1, sx)
    upper = upper_half()
    for e in range(rows // 4 + 1):
        low = mcol_ref[pl.ds(4 * e - 1, 1), :] if e > 0 else rb[pairs, 0:1]
        high = mcol_ref[pl.ds(4 * e, 1), :] if e <= last else ra[pairs, 0:1]
        total = 1.0 / (low + high)
        if e > 0:
            inv_ref[pl.ds(4 * e - 1, 1), :] = total
        if e <= last:
            inv_ref[pl.ds(4 * e, 1), :] = total
            inv_ref[pl.ds(4 * e + 1, 2), :] = 1.0 / mcol_ref[pl.ds(4 * e + 1, 2), :]

    def band(e, carry):
        def load(row, a, p):
            v = whole_point(a_ref, rb, ra, before, after, row, a, p, e, last, pairs)
            return v * spread(inv_ref, row, p, upper)

        laplace_band(load, e, pairs, (s0, s1, sx), out_ref, colf_ref, coll_ref)
        return carry

    lax.fori_loop(0, rows // 4, band, 0)
    col_edges(out_ref, rows, pairs, colf_ref, coll_ref)


def last_kernel(a_ref, before, after, rb, ra, inv_ref, out_ref):
    rows, pairs = a_ref.shape[:2]
    last = rows // 4 - 1
    upper = upper_half()

    def band(e, carry):
        for a in range(4):
            for p in range(pairs):
                row = 4 * e + a
                v = whole_point(a_ref, rb, ra, before, after, row, a, p, e, last, pairs)
                out_ref[row, p] = v * spread(inv_ref, row, p, upper)
        return carry

    lax.fori_loop(0, rows // 4, band, 0)


def exchange(first, last, axis):
    devices = lax.axis_size(axis)
    up = [(i, (i + 1) % devices) for i in range(devices)]
    down = [(j, i) for i, j in up]
    return lax.ppermute(last, axis, up), lax.ppermute(first, axis, down)


def call(kernel, outs, scratch, cost, *args):
    return pl.pallas_call(
        kernel,
        out_shape=[jax.ShapeDtypeStruct(s, F32) for s in outs],
        in_specs=[pl.BlockSpec(memory_space=VMEM)] * len(args),
        out_specs=[pl.BlockSpec(memory_space=VMEM)] * len(outs),
        scratch_shapes=[VMEM(s, F32) for s in scratch],
        cost_estimate=pl.CostEstimate(flops=cost, bytes_accessed=cost // 4, transcendentals=0),
    )(*args)


def edge_call(kernel, outs, scratch, array, *args):
    rows, pairs = array.shape[:2]

    def whole(x):
        return pl.BlockSpec(x.shape, lambda i, n=len(x.shape): (0,) * n)

    return pl.pallas_call(
        kernel,
        grid=(1,),
        out_shape=[jax.ShapeDtypeStruct(s, F32) for s in outs],
        in_specs=[
            pl.BlockSpec((1, pairs, 8, 128), lambda i: (0, 0, 0, 0)),
            pl.BlockSpec((1, pairs, 8, 128), lambda i: (rows - 1, 0, 0, 0)),
        ] + [whole(x) for x in args],
        out_specs=[whole(jax.ShapeDtypeStruct(s, F32)) for s in outs],
        scratch_shapes=[VMEM(s, F32) for s in scratch],
    )(array, array, *args)


def shards(fields, metric_diag, metric_cross, point_mass):
    nfield, rows, cols, nlev = fields.shape
    pairs = cols // 2
    u = fields.transpose(1, 2, 0, 3).reshape(rows, pairs, 2 * nfield, nlev)
    md = metric_diag.transpose(1, 0, 2)
    full = (rows, pairs, 8, 128)
    line = (rows, 128)
    tall = ((rows + 7) // 8 * 8, 128)
    flops = 60 * rows * pairs * 8 * 128

    a1, cf, cl = call(
        first_kernel, [full] + [(rows + rows // 4, 4, 128)] * 2, [line] * 4, flops,
        u, md, metric_cross, point_mass,
    )
    cb, ca = exchange(cf, cl, "col")
    rf, rl, mcol = edge_call(
        edge_kernel_mass, [(pairs + 1, 8, 128)] * 2 + [line], [tall] * 3, a1, cb, ca, point_mass
    )
    rb, ra = exchange(rf, rl, "face")
    a2, cf, cl, inv = call(
        second_kernel, [full] + [(rows, 4, 128)] * 2 + [line], [line] * 3, flops,
        a1, cb, ca, rb, ra, mcol, md, metric_cross,
    )
    cb, ca = exchange(cf, cl, "col")
    rf, rl = edge_call(
        functools.partial(edge_kernel, rows=rows, pairs=pairs),
        [(pairs, 8, 128)] * 2, [], a2, cb, ca,
    )
    rb, ra = exchange(rf, rl, "face")
    (out,) = call(last_kernel, [full], [], flops // 10, a2, cb, ca, rb, ra, inv)
    return out.reshape(rows, cols, nfield, nlev).transpose(2, 0, 1, 3)


def solution(mesh):
    return jax.shard_map(
        shards,
        mesh=mesh,
        in_specs=(
            P(None, "face", "col", None),
            P(None, "face", "col"),
            P("face", "col"),
            P("face", "col"),
        ),
        out_specs=P(None, "face", "col", None),
        check_vma=False,
    )
```

```python
import jax
import jax.numpy as jnp
import numpy as np
from jax import lax
from jax.experimental import pallas as pl
from jax.experimental.pallas import tpu as pltpu
from jax.sharding import PartitionSpec as P

F32 = jnp.float32
VMEM = pltpu.VMEM
VMEM_LIMIT = 6 * 2**20


def derivative_table():
    small = 1.0 / np.sqrt(5.0)
    nodes = np.array([-1.0, -small, small, 1.0])
    count = nodes.shape[0]
    weights = np.array(
        [np.prod([nodes[a] - nodes[k] for k in range(count) if k != a]) for a in range(count)]
    )
    table = np.zeros((count, count))
    for a in range(count):
        for b in range(count):
            if a == b:
                table[a, b] = np.sum([1.0 / (nodes[a] - nodes[k]) for k in range(count) if k != a])
            else:
                table[a, b] = weights[a] / weights[b] / (nodes[a] - nodes[b])
    return table.astype(np.float32)


D = derivative_table()


def upper_half():
    return lax.broadcasted_iota(jnp.int32, (8, 128), 0) >= 4


def swap(v):
    return pltpu.roll(v, 4, 0)


def col_coefs(table, upper):
    def vec(low, high):
        return jnp.where(upper, float(high), float(low)).astype(F32)

    return [
        [
            (vec(table[2 * h, 2 * k], table[2 * h + 1, 2 * k + 1]),
             vec(table[2 * h, 2 * k + 1], table[2 * h + 1, 2 * k]))
            for k in range(2)
        ]
        for h in range(2)
    ]


def col_apply(coefs, pair):
    swapped = [swap(v) for v in pair]
    out = []
    for h in range(2):
        (s0, x0), (s1, x1) = coefs[h]
        out.append((s0 * pair[0] + x0 * swapped[0]) + (s1 * pair[1] + x1 * swapped[1]))
    return out


def row_apply(table, vs):
    out = []
    for a in range(4):
        terms = [float(table[a, b]) * vs[b] for b in range(4)]
        out.append((terms[0] + terms[1]) + (terms[2] + terms[3]))
    return out


def spread(ref, row, pair, upper):
    line = jnp.broadcast_to(ref[pl.ds(row, 1), :], (8, 128))
    index = jnp.where(upper, 2 * pair + 1, 2 * pair).astype(jnp.int32)
    return jnp.take_along_axis(line, index, axis=1, mode="promise_in_bounds")


def element(load, base, g, mets, upper, fwd, bwd):
    d0, d1, dx = mets
    u = [[load(base + a, a, 2 * g + h) for h in range(2)] for a in range(4)]
    gx = [row_apply(D, [u[b][h] for b in range(4)]) for h in range(2)]
    fx = [[None] * 2 for _ in range(4)]
    wy = [None] * 4
    for a in range(4):
        gy = col_apply(fwd, u[a])
        fy = [None] * 2
        for h in range(2):
            p = 2 * g + h
            cross = spread(dx, base + a, p, upper)
            fx[a][h] = spread(d0, base + a, p, upper) * gx[h][a] + cross * gy[h]
            fy[h] = cross * gx[h][a] + spread(d1, base + a, p, upper) * gy[h]
        wy[a] = col_apply(bwd, fy)
    done = [[None] * 2 for _ in range(4)]
    for h in range(2):
        wx = row_apply(-D.T, [fx[b][h] for b in range(4)])
        for a in range(4):
            done[a][h] = wx[a] + wy[a][h]
    return done


def laplace_band(made, base, put, pairs, upper):
    lower = jnp.logical_not(upper)
    previous = None
    for g in range(pairs // 2):
        done = made(g)
        if previous is not None:
            for a in range(4):
                left, right = previous[a], done[a][0]
                put(base + a, 2 * g - 1, left + jnp.where(upper, swap(right), 0.0))
                done[a][0] = right + jnp.where(lower, swap(left), 0.0)
        for a in range(4):
            put(base + a, 2 * g, done[a][0])
        previous = [done[a][1] for a in range(4)]
    for a in range(4):
        put(base + a, pairs - 1, previous[a])


def join_rows(ref, row, pairs):
    for p in range(pairs):
        total = ref[row - 1, p] + ref[row, p]
        ref[row - 1, p] = total
        ref[row, p] = total


def constants():
    upper = upper_half()
    return upper, col_coefs(D, upper), col_coefs(-D.T, upper)


def odd(axis):
    return lax.rem(lax.axis_index(axis), 2) == 1


def put_slots(is_odd, index, first, last, slot_a, slot_b):
    slot_a[index] = jnp.where(is_odd, first, last)
    slot_b[index] = jnp.where(is_odd, last, first)


def first_edges(
    u_hbm, md_hbm, mc_hbm, mass_hbm,
    edge_ref, ca_ref, cb_ref, s0, s1, sx, sm, u_ref, md_v, mc_v, mass_v, sem,
):
    rows, pairs = u_ref.shape[:2]
    cols = 2 * pairs
    bands = rows // 4

    def chunk(e):
        part = pl.ds(4 * e, 4)
        return pltpu.make_async_copy(u_hbm.at[part], u_ref.at[part], sem.at[e])

    small = [
        pltpu.make_async_copy(source, dest, sem.at[bands + k])
        for k, (source, dest) in enumerate(
            ((md_hbm, md_v), (mc_hbm, mc_v), (mass_hbm, mass_v))
        )
    ]
    for copy in small:
        copy.start()
    for e in range(bands):
        chunk(e).start()
    for copy in small:
        copy.wait()
    s0[:, 0:cols] = md_v[:, 0, :]
    s1[:, 0:cols] = md_v[:, 1, :]
    sx[:, 0:cols] = mc_v[...]
    sm[...] = jnp.ones_like(sm)
    sm[:, 0:cols] = mass_v[...]
    upper, fwd, bwd = constants()

    def band(e, carry):
        chunk(e).wait()
        for k, g in enumerate((0, pairs // 2 - 1)):
            done = element(
                lambda row, a, p: u_ref[row, p], 4 * e, g, (s0, s1, sx), upper, fwd, bwd
            )
            for a in range(4):
                for h in range(2):
                    edge_ref[4 * e + a, 2 * k + h] = done[a][h]
        return carry

    lax.fori_loop(0, bands, band, 0)
    is_odd = odd("col")
    firsts = [edge_ref[r, 0] for r in range(rows)]
    lasts = [edge_ref[r, 3] for r in range(rows)]
    for r in range(rows):
        f, l = firsts[r], lasts[r]
        other = r - 1 if r % 4 == 0 else r + 1 if r % 4 == 3 else -1
        if 0 <= other < rows:
            f, l = f + firsts[other], l + lasts[other]
        put_slots(is_odd, r, f[0:4], l[4:8], ca_ref, cb_ref)
    for q in range(bands):
        part = sm[pl.ds(4 * q, 4), :]
        ca_ref[rows + q] = part
        cb_ref[rows + q] = part


def first_middle(u_ref, edge_ref, s0, s1, sx, out_ref, rowf_ref, rowl_ref):
    rows, pairs = u_ref.shape[:2]
    last = pairs // 2 - 1
    upper, fwd, bwd = constants()

    def band(e, carry):
        base = 4 * e

        def made(g):
            if g in (0, last):
                k = 0 if g == 0 else 2
                return [[edge_ref[base + a, k + h] for h in range(2)] for a in range(4)]
            return element(
                lambda row, a, p: u_ref[row, p], base, g, (s0, s1, sx), upper, fwd, bwd
            )

        def put(row, p, v):
            out_ref[row, p] = v

        laplace_band(made, base, put, pairs, upper)

        @pl.when(e > 0)
        def _():
            join_rows(out_ref, base, pairs)

        return carry

    lax.fori_loop(0, rows // 4, band, 0)
    for p in range(pairs):
        rowf_ref[p] = out_ref[0, p]
        rowl_ref[p] = out_ref[rows - 1, p]


def row_slots(rowf, rowl, ra, rb, fa_ref, fb_ref, low_ref, high_ref):
    pairs, rows = rowf.shape[0], low_ref.shape[0]
    col_odd, face_odd = odd("col"), odd("face")
    zero = jnp.zeros((4, 128), F32)
    for r in range(rows):
        a, b = ra[r], rb[r]
        low = jnp.concatenate([jnp.where(col_odd, a, b), zero], axis=0)
        high = jnp.concatenate([zero, jnp.where(col_odd, b, a)], axis=0)
        low_ref[r] = low
        high_ref[r] = high
    for p in range(pairs):
        f, l = rowf[p], rowl[p]
        if p == 0:
            f, l = f + low_ref[0], l + low_ref[rows - 1]
        if p == pairs - 1:
            f, l = f + high_ref[0], l + high_ref[rows - 1]
        put_slots(face_odd, p, f, l, fa_ref, fb_ref)


def row_slots_mass(
    rowf, rowl, ra, rb, mass, fa_ref, fb_ref, low_ref, high_ref, mcol_ref, sb, sa, sm,
):
    pairs, rows = rowf.shape[0], mass.shape[0]
    cols = 2 * pairs
    row_slots(rowf, rowl, ra, rb, fa_ref, fb_ref, low_ref, high_ref)
    col_odd = odd("col")
    for q in range(rows // 4):
        part = pl.ds(4 * q, 4)
        a, b = ra[rows + q], rb[rows + q]
        sb[part, :] = jnp.where(col_odd, a, b)
        sa[part, :] = jnp.where(col_odd, b, a)
    sm[...] = jnp.ones_like(sm)
    sm[pl.ds(0, rows), :] = mass[...]
    m = sm[...]
    lane = lax.broadcasted_iota(jnp.int32, m.shape, 1)
    prev = jnp.where(lane == 0, pltpu.roll(sb[...], 128 - (cols - 1), 1), pltpu.roll(m, 1, 1))
    following = jnp.where(
        lane == cols - 1, pltpu.roll(sa[...], cols - 1, 1), pltpu.roll(m, 127, 1)
    )
    m = m + jnp.where(lane % 4 == 0, prev, 0.0) + jnp.where(lane % 4 == 3, following, 0.0)
    sm[...] = m
    mcol_ref[...] = sm[pl.ds(0, rows), :]
    first = jnp.broadcast_to(sm[pl.ds(0, 1), :], (8, 128))
    final = jnp.broadcast_to(sm[pl.ds(rows - 1, 1), :], (8, 128))
    put_slots(odd("face"), pairs, first, final, fa_ref, fb_ref)


def with_sides(a_ref, low_ref, high_ref, row, p):
    v = a_ref[row, p]
    if p == 0:
        v = v + low_ref[row]
    if p == a_ref.shape[1] - 1:
        v = v + high_ref[row]
    return v


def second_middle(a_ref, low_ref, high_ref, mcol_ref, s0, s1, sx, out_ref, inv_ref):
    rows, pairs = a_ref.shape[:2]
    bands = rows // 4
    upper, fwd, bwd = constants()
    inv_ref[pl.ds(0, 1), :] = mcol_ref[pl.ds(0, 1), :]
    inv_ref[pl.ds(rows - 1, 1), :] = mcol_ref[pl.ds(rows - 1, 1), :]
    for e in range(bands):
        inv_ref[pl.ds(4 * e + 1, 2), :] = 1.0 / mcol_ref[pl.ds(4 * e + 1, 2), :]
        if e > 0:
            total = 1.0 / (mcol_ref[pl.ds(4 * e - 1, 1), :] + mcol_ref[pl.ds(4 * e, 1), :])
            inv_ref[pl.ds(4 * e - 1, 1), :] = total
            inv_ref[pl.ds(4 * e, 1), :] = total

    def band(e, carry):
        base = 4 * e

        def load(row, a, p):
            v = with_sides(a_ref, low_ref, high_ref, row, p)
            return v * spread(inv_ref, row, p, upper)

        def put(row, p, v):
            out_ref[row - 4, p] = v

        laplace_band(
            lambda g: element(load, base, g, (s0, s1, sx), upper, fwd, bwd),
            base, put, pairs, upper,
        )

        @pl.when(e > 1)
        def _():
            join_rows(out_ref, base - 4, pairs)

        return carry

    lax.fori_loop(1, bands - 1, band, 0)


def second_ends(
    a_ref, mid_ref, low_ref, high_ref, fa, fb, ra, rb, invm_ref, s0, s1, sx,
    out_ref, rowf_ref, rowl_ref, ca_ref, cb_ref, inv_ref, tf, tl,
):
    rows, pairs = a_ref.shape[:2]
    last = rows // 4 - 1
    upper, fwd, bwd = constants()
    face_odd = odd("face")
    for p in range(pairs + 1):
        total_a, total_b = fa[p] + ra[p], fb[p] + rb[p]
        tf[p] = jnp.where(face_odd, total_a, total_b)
        tl[p] = jnp.where(face_odd, total_b, total_a)
    inv_ref[...] = invm_ref[...]
    inv_ref[pl.ds(0, 1), :] = 1.0 / tf[pairs, 0:1]
    inv_ref[pl.ds(rows - 1, 1), :] = 1.0 / tl[pairs, 0:1]

    def band(k, carry):
        base = 4 * last * k

        def load(row, a, p):
            v = with_sides(a_ref, low_ref, high_ref, row, p)
            if a == 0:
                v = jnp.where(k == 0, tf[p], v)
            if a == 3:
                v = jnp.where(k == 1, tl[p], v)
            return v * spread(inv_ref, row, p, upper)

        def put(row, p, v):
            out_ref[row, p] = v

        laplace_band(
            lambda g: element(load, base, g, (s0, s1, sx), upper, fwd, bwd),
            base, put, pairs, upper,
        )
        return carry

    lax.fori_loop(0, 2, band, 0)

    def carry_over(r, carry):
        for p in range(pairs):
            out_ref[r, p] = mid_ref[r - 4, p]
        return carry

    lax.fori_loop(4, rows - 4, carry_over, 0)
    join_rows(out_ref, 4, pairs)
    join_rows(out_ref, rows - 4, pairs)
    for p in range(pairs):
        rowf_ref[p] = out_ref[0, p]
        rowl_ref[p] = out_ref[rows - 1, p]
    is_odd = odd("col")
    for r in range(rows):
        put_slots(is_odd, r, out_ref[r, 0][0:4], out_ref[r, pairs - 1][4:8], ca_ref, cb_ref)


def last_middle(a_ref, low_ref, high_ref, inv_ref, out_hbm, buf, sem):
    rows, pairs = a_ref.shape[:2]
    bands = rows // 4
    upper = upper_half()
    copies = []
    for e in range(bands):
        start = 1 if e == 0 else 4 * e
        stop = rows - 1 if e == bands - 1 else 4 * e + 4
        for row in range(start, stop):
            for p in range(pairs):
                v = with_sides(a_ref, low_ref, high_ref, row, p)
                buf[row, p] = v * spread(inv_ref, row, p, upper)
        part = pl.ds(start, stop - start)
        copies.append(pltpu.make_async_copy(buf.at[part], out_hbm.at[part], sem.at[e]))
        copies[-1].start()
    for copy in copies:
        copy.wait()


def last_ends(held, fa, fb, ra, rb, inv_ref, out_hbm, buf, sem):
    rows, pairs = out_hbm.shape[:2]
    upper = upper_half()
    face_odd = odd("face")
    for p in range(pairs):
        total_a, total_b = fa[p] + ra[p], fb[p] + rb[p]
        buf[0, p] = jnp.where(face_odd, total_a, total_b) * spread(inv_ref, 0, p, upper)
        buf[1, p] = jnp.where(face_odd, total_b, total_a) * spread(inv_ref, rows - 1, p, upper)
    copies = [
        pltpu.make_async_copy(buf.at[k], out_hbm.at[row], sem.at[k])
        for k, row in enumerate((0, rows - 1))
    ]
    for copy in copies:
        copy.start()
    for copy in copies:
        copy.wait()


def exchange(slot_a, slot_b, axis):
    n = lax.axis_size(axis)
    pairs_a = [(i, i ^ 1) for i in range(n)]
    pairs_b = [(i, (i + 1) % n if i % 2 else (i - 1) % n) for i in range(n)]
    got_b = lax.ppermute(slot_b, axis, pairs_b)
    got_a = lax.ppermute(slot_a, axis, pairs_a)
    return got_a, got_b


def call(kernel, outs, cost, args, scratch=(), far_in=0, far_out=False, alias=None):
    far = pl.BlockSpec(memory_space=pltpu.HBM)
    return pl.pallas_call(
        kernel,
        out_shape=[jax.ShapeDtypeStruct(s, F32) for s in outs],
        in_specs=[far] * far_in + [pl.BlockSpec()] * (len(args) - far_in),
        out_specs=[far if far_out else pl.BlockSpec()] * len(outs),
        scratch_shapes=scratch,
        input_output_aliases=alias or {},
        cost_estimate=pl.CostEstimate(flops=cost, bytes_accessed=cost // 4, transcendentals=0),
        compiler_params=pltpu.CompilerParams(vmem_limit_bytes=VMEM_LIMIT),
    )(*args)


def shards(fields, metric_diag, metric_cross, point_mass):
    nfield, rows, cols, nlev = fields.shape
    pairs, bands = cols // 2, rows // 4
    u = fields.transpose(1, 2, 0, 3).reshape(rows, pairs, 2 * nfield, nlev)
    md = metric_diag.transpose(1, 0, 2)
    full = (rows, pairs, 8, 128)
    edge = (pairs, 8, 128)
    heavy = (pairs + 1, 8, 128)
    side = (rows, 8, 128)
    line = (rows, 128)
    tall = ((rows + 7) // 8 * 8, 128)
    flops = 60 * rows * pairs * 8 * 128

    ends, ca, cb, s0, s1, sx, sm, uv = call(
        first_edges,
        [(rows, 4, 8, 128)] + [(rows + bands, 4, 128)] * 2 + [line] * 4 + [full],
        flops * 2 // 5,
        [u, md, metric_cross, point_mass],
        [VMEM(md.shape, F32), VMEM((rows, cols), F32), VMEM((rows, cols), F32),
         pltpu.SemaphoreType.DMA((bands + 3,))],
        far_in=4,
    )
    ga, gb = exchange(ca, cb, "col")
    a1, rf, rl = call(first_middle, [full, edge, edge], flops * 3 // 5, [uv, ends, s0, s1, sx])
    fa, fb, low, high, mcol = call(
        row_slots_mass, [heavy, heavy, side, side, line], flops // 50,
        [rf, rl, ga, gb, sm], [VMEM(tall, F32)] * 3,
    )
    ra, rb = exchange(fa, fb, "face")
    mid, invm = call(
        second_middle, [(rows - 8, pairs, 8, 128), line], flops * 3 // 5,
        [a1, low, high, mcol, s0, s1, sx],
    )
    a2, rf, rl, ca, cb, inv = call(
        second_ends, [full, edge, edge, (rows, 4, 128), (rows, 4, 128), line], flops * 2 // 5,
        [a1, mid, low, high, fa, fb, ra, rb, invm, s0, s1, sx], [VMEM(heavy, F32)] * 2,
    )
    ga, gb = exchange(ca, cb, "col")
    fa, fb, low, high = call(
        row_slots, [edge, edge, side, side], flops // 50, [rf, rl, ga, gb]
    )
    ra, rb = exchange(fa, fb, "face")
    (out,) = call(
        last_middle, [full], flops // 5, [a2, low, high, inv],
        [VMEM(full, F32), pltpu.SemaphoreType.DMA((bands,))], far_out=True,
    )
    (out,) = call(
        last_ends, [full], flops // 50, [out, fa, fb, ra, rb, inv],
        [VMEM((2,) + edge, F32), pltpu.SemaphoreType.DMA((2,))],
        far_in=1, far_out=True, alias={0: 0},
    )
    return out.reshape(rows, cols, nfield, nlev).transpose(2, 0, 1, 3)


def solution(mesh):
    return jax.shard_map(
        shards,
        mesh=mesh,
        in_specs=(
            P(None, "face", "col", None),
            P(None, "face", "col"),
            P("face", "col"),
            P("face", "col"),
        ),
        out_specs=P(None, "face", "col", None),
        check_vma=False,
    )
```

```python
import jax
import jax.numpy as jnp
import numpy as np
from jax import lax
from jax.experimental import pallas as pl
from jax.experimental.pallas import tpu as pltpu
from jax.sharding import PartitionSpec as P

F32 = jnp.float32
VMEM = pltpu.VMEM
VMEM_LIMIT = 6 * 2**20


def derivative_table():
    small = 1.0 / np.sqrt(5.0)
    nodes = np.array([-1.0, -small, small, 1.0])
    count = nodes.shape[0]
    weights = np.array(
        [np.prod([nodes[a] - nodes[k] for k in range(count) if k != a]) for a in range(count)]
    )
    table = np.zeros((count, count))
    for a in range(count):
        for b in range(count):
            if a == b:
                table[a, b] = np.sum([1.0 / (nodes[a] - nodes[k]) for k in range(count) if k != a])
            else:
                table[a, b] = weights[a] / weights[b] / (nodes[a] - nodes[b])
    return table.astype(np.float32)


D = derivative_table()


def upper_half():
    return lax.broadcasted_iota(jnp.int32, (8, 128), 0) >= 4


def swap(v):
    return pltpu.roll(v, 4, 0)


def col_coefs(table, upper):
    def vec(low, high):
        return jnp.where(upper, float(high), float(low)).astype(F32)

    return [
        [
            (vec(table[2 * h, 2 * k], table[2 * h + 1, 2 * k + 1]),
             vec(table[2 * h, 2 * k + 1], table[2 * h + 1, 2 * k]))
            for k in range(2)
        ]
        for h in range(2)
    ]


def col_apply(coefs, pair):
    swapped = [swap(v) for v in pair]
    out = []
    for h in range(2):
        (s0, x0), (s1, x1) = coefs[h]
        out.append((s0 * pair[0] + x0 * swapped[0]) + (s1 * pair[1] + x1 * swapped[1]))
    return out


def row_apply(table, vs):
    out = []
    for a in range(4):
        terms = [float(table[a, b]) * vs[b] for b in range(4)]
        out.append((terms[0] + terms[1]) + (terms[2] + terms[3]))
    return out


def spread(ref, row, pair, upper):
    line = jnp.broadcast_to(ref[pl.ds(row, 1), :], (8, 128))
    index = jnp.where(upper, 2 * pair + 1, 2 * pair).astype(jnp.int32)
    return jnp.take_along_axis(line, index, axis=1, mode="promise_in_bounds")


def element(load, base, g, mets, upper, fwd, bwd):
    d0, d1, dx = mets
    u = [[load(base + a, a, 2 * g + h) for h in range(2)] for a in range(4)]
    gx = [row_apply(D, [u[b][h] for b in range(4)]) for h in range(2)]
    fx = [[None] * 2 for _ in range(4)]
    wy = [None] * 4
    for a in range(4):
        gy = col_apply(fwd, u[a])
        fy = [None] * 2
        for h in range(2):
            p = 2 * g + h
            cross = spread(dx, base + a, p, upper)
            fx[a][h] = spread(d0, base + a, p, upper) * gx[h][a] + cross * gy[h]
            fy[h] = cross * gx[h][a] + spread(d1, base + a, p, upper) * gy[h]
        wy[a] = col_apply(bwd, fy)
    done = [[None] * 2 for _ in range(4)]
    for h in range(2):
        wx = row_apply(-D.T, [fx[b][h] for b in range(4)])
        for a in range(4):
            done[a][h] = wx[a] + wy[a][h]
    return done


def laplace_band(made, base, put, pairs, upper):
    lower = jnp.logical_not(upper)
    previous = None
    for g in range(pairs // 2):
        done = made(g)
        if previous is not None:
            for a in range(4):
                left, right = previous[a], done[a][0]
                put(base + a, 2 * g - 1, left + jnp.where(upper, swap(right), 0.0))
                done[a][0] = right + jnp.where(lower, swap(left), 0.0)
        for a in range(4):
            put(base + a, 2 * g, done[a][0])
        previous = [done[a][1] for a in range(4)]
    for a in range(4):
        put(base + a, pairs - 1, previous[a])


def join_rows(ref, row, pairs):
    for p in range(pairs):
        total = ref[row - 1, p] + ref[row, p]
        ref[row - 1, p] = total
        ref[row, p] = total


def constants():
    upper = upper_half()
    return upper, col_coefs(D, upper), col_coefs(-D.T, upper)


def odd(axis):
    return lax.rem(lax.axis_index(axis), 2) == 1


def put_slots(is_odd, index, first, last, slot_a, slot_b):
    slot_a[index] = jnp.where(is_odd, first, last)
    slot_b[index] = jnp.where(is_odd, last, first)


def first_edges(
    u_hbm, md_hbm, mc_hbm, mass_hbm,
    edge_ref, ca_ref, cb_ref, s0, s1, sx, sm, u_ref, md_v, mc_v, mass_v, sem,
):
    rows, pairs = u_ref.shape[:2]
    cols = 2 * pairs
    bands = rows // 4

    def chunk(e):
        part = pl.ds(4 * e, 4)
        return pltpu.make_async_copy(u_hbm.at[part], u_ref.at[part], sem.at[e])

    small = [
        pltpu.make_async_copy(source, dest, sem.at[bands + k])
        for k, (source, dest) in enumerate(
            ((md_hbm, md_v), (mc_hbm, mc_v), (mass_hbm, mass_v))
        )
    ]
    for copy in small:
        copy.start()
    for e in range(bands):
        chunk(e).start()
    for copy in small:
        copy.wait()
    s0[:, 0:cols] = md_v[:, 0, :]
    s1[:, 0:cols] = md_v[:, 1, :]
    sx[:, 0:cols] = mc_v[...]
    sm[...] = jnp.ones_like(sm)
    sm[:, 0:cols] = mass_v[...]
    upper, fwd, bwd = constants()

    def band(e, carry):
        chunk(e).wait()
        for k, g in enumerate((0, pairs // 2 - 1)):
            done = element(
                lambda row, a, p: u_ref[row, p], 4 * e, g, (s0, s1, sx), upper, fwd, bwd
            )
            for a in range(4):
                for h in range(2):
                    edge_ref[4 * e + a, 2 * k + h] = done[a][h]
        return carry

    lax.fori_loop(0, bands, band, 0)
    is_odd = odd("col")
    firsts = [edge_ref[r, 0] for r in range(rows)]
    lasts = [edge_ref[r, 3] for r in range(rows)]
    for r in range(rows):
        f, l = firsts[r], lasts[r]
        other = r - 1 if r % 4 == 0 else r + 1 if r % 4 == 3 else -1
        if 0 <= other < rows:
            f, l = f + firsts[other], l + lasts[other]
        put_slots(is_odd, r, f[0:4], l[4:8], ca_ref, cb_ref)
    for q in range(bands):
        part = sm[pl.ds(4 * q, 4), :]
        ca_ref[rows + q] = part
        cb_ref[rows + q] = part


def first_middle(u_ref, edge_ref, s0, s1, sx, out_ref, rowf_ref, rowl_ref):
    rows, pairs = u_ref.shape[:2]
    last = pairs // 2 - 1
    upper, fwd, bwd = constants()

    def band(e, carry):
        base = 4 * e

        def made(g):
            if g in (0, last):
                k = 0 if g == 0 else 2
                return [[edge_ref[base + a, k + h] for h in range(2)] for a in range(4)]
            return element(
                lambda row, a, p: u_ref[row, p], base, g, (s0, s1, sx), upper, fwd, bwd
            )

        def put(row, p, v):
            out_ref[row, p] = v

        laplace_band(made, base, put, pairs, upper)

        @pl.when(e > 0)
        def _():
            join_rows(out_ref, base, pairs)

        return carry

    lax.fori_loop(0, rows // 4, band, 0)
    for p in range(pairs):
        rowf_ref[p] = out_ref[0, p]
        rowl_ref[p] = out_ref[rows - 1, p]


def row_slots(rowf, rowl, rb, ra, fb_ref, fa_ref, low_ref, high_ref):
    pairs, rows = rowf.shape[0], low_ref.shape[0]
    col_odd, face_odd = odd("col"), odd("face")
    zero = jnp.zeros((4, 128), F32)
    for r in range(rows):
        a, b = ra[r], rb[r]
        low = jnp.concatenate([jnp.where(col_odd, a, b), zero], axis=0)
        high = jnp.concatenate([zero, jnp.where(col_odd, b, a)], axis=0)
        low_ref[r] = low
        high_ref[r] = high
    for p in range(pairs):
        f, l = rowf[p], rowl[p]
        if p == 0:
            f, l = f + low_ref[0], l + low_ref[rows - 1]
        if p == pairs - 1:
            f, l = f + high_ref[0], l + high_ref[rows - 1]
        put_slots(face_odd, p, f, l, fa_ref, fb_ref)


def row_slots_mass(
    rowf, rowl, rb, ra, mass, fb_ref, fa_ref, low_ref, high_ref, mcol_ref, sb, sa, sm,
):
    pairs, rows = rowf.shape[0], mass.shape[0]
    cols = 2 * pairs
    row_slots(rowf, rowl, rb, ra, fb_ref, fa_ref, low_ref, high_ref)
    col_odd = odd("col")
    for q in range(rows // 4):
        part = pl.ds(4 * q, 4)
        a, b = ra[rows + q], rb[rows + q]
        sb[part, :] = jnp.where(col_odd, a, b)
        sa[part, :] = jnp.where(col_odd, b, a)
    sm[...] = jnp.ones_like(sm)
    sm[pl.ds(0, rows), :] = mass[...]
    m = sm[...]
    lane = lax.broadcasted_iota(jnp.int32, m.shape, 1)
    prev = jnp.where(lane == 0, pltpu.roll(sb[...], 128 - (cols - 1), 1), pltpu.roll(m, 1, 1))
    following = jnp.where(
        lane == cols - 1, pltpu.roll(sa[...], cols - 1, 1), pltpu.roll(m, 127, 1)
    )
    m = m + jnp.where(lane % 4 == 0, prev, 0.0) + jnp.where(lane % 4 == 3, following, 0.0)
    sm[...] = m
    mcol_ref[...] = sm[pl.ds(0, rows), :]
    first = jnp.broadcast_to(sm[pl.ds(0, 1), :], (8, 128))
    final = jnp.broadcast_to(sm[pl.ds(rows - 1, 1), :], (8, 128))
    put_slots(odd("face"), pairs, first, final, fa_ref, fb_ref)


def with_sides(a_ref, low_ref, high_ref, row, p):
    v = a_ref[row, p]
    if p == 0:
        v = v + low_ref[row]
    if p == a_ref.shape[1] - 1:
        v = v + high_ref[row]
    return v


def second_middle(a_ref, low_ref, high_ref, mcol_ref, s0, s1, sx, out_ref, inv_ref):
    rows, pairs = a_ref.shape[:2]
    bands = rows // 4
    upper, fwd, bwd = constants()
    inv_ref[pl.ds(0, 1), :] = mcol_ref[pl.ds(0, 1), :]
    inv_ref[pl.ds(rows - 1, 1), :] = mcol_ref[pl.ds(rows - 1, 1), :]
    for e in range(bands):
        inv_ref[pl.ds(4 * e + 1, 2), :] = 1.0 / mcol_ref[pl.ds(4 * e + 1, 2), :]
        if e > 0:
            total = 1.0 / (mcol_ref[pl.ds(4 * e - 1, 1), :] + mcol_ref[pl.ds(4 * e, 1), :])
            inv_ref[pl.ds(4 * e - 1, 1), :] = total
            inv_ref[pl.ds(4 * e, 1), :] = total

    def band(e, carry):
        base = 4 * e

        def load(row, a, p):
            v = with_sides(a_ref, low_ref, high_ref, row, p)
            return v * spread(inv_ref, row, p, upper)

        def put(row, p, v):
            out_ref[row - 4, p] = v

        laplace_band(
            lambda g: element(load, base, g, (s0, s1, sx), upper, fwd, bwd),
            base, put, pairs, upper,
        )

        @pl.when(e > 1)
        def _():
            join_rows(out_ref, base - 4, pairs)

        return carry

    lax.fori_loop(1, bands - 1, band, 0)


def second_ends(
    a_ref, mid_ref, low_ref, high_ref, fb, fa, rb, ra, invm_ref, s0, s1, sx,
    out_ref, rowf_ref, rowl_ref, ca_ref, cb_ref, inv_ref, tf, tl,
):
    rows, pairs = a_ref.shape[:2]
    last = rows // 4 - 1
    upper, fwd, bwd = constants()
    face_odd = odd("face")
    for p in range(pairs + 1):
        total_a, total_b = fa[p] + ra[p], fb[p] + rb[p]
        tf[p] = jnp.where(face_odd, total_a, total_b)
        tl[p] = jnp.where(face_odd, total_b, total_a)
    inv_ref[...] = invm_ref[...]
    inv_ref[pl.ds(0, 1), :] = 1.0 / tf[pairs, 0:1]
    inv_ref[pl.ds(rows - 1, 1), :] = 1.0 / tl[pairs, 0:1]

    def band(k, carry):
        base = 4 * last * k

        def load(row, a, p):
            v = with_sides(a_ref, low_ref, high_ref, row, p)
            if a == 0:
                v = jnp.where(k == 0, tf[p], v)
            if a == 3:
                v = jnp.where(k == 1, tl[p], v)
            return v * spread(inv_ref, row, p, upper)

        def put(row, p, v):
            out_ref[row, p] = v

        laplace_band(
            lambda g: element(load, base, g, (s0, s1, sx), upper, fwd, bwd),
            base, put, pairs, upper,
        )
        return carry

    lax.fori_loop(0, 2, band, 0)

    def carry_over(r, carry):
        for p in range(pairs):
            out_ref[r, p] = mid_ref[r - 4, p]
        return carry

    lax.fori_loop(4, rows - 4, carry_over, 0)
    join_rows(out_ref, 4, pairs)
    join_rows(out_ref, rows - 4, pairs)
    for p in range(pairs):
        rowf_ref[p] = out_ref[0, p]
        rowl_ref[p] = out_ref[rows - 1, p]
    is_odd = odd("col")
    for r in range(rows):
        put_slots(is_odd, r, out_ref[r, 0][0:4], out_ref[r, pairs - 1][4:8], ca_ref, cb_ref)


def last_middle(a_ref, low_ref, high_ref, inv_ref, out_hbm, buf, sem):
    rows, pairs = a_ref.shape[:2]
    bands = rows // 4
    upper = upper_half()
    copies = []
    for e in range(bands):
        start = 1 if e == 0 else 4 * e
        stop = rows - 1 if e == bands - 1 else 4 * e + 4
        for row in range(start, stop):
            for p in range(pairs):
                v = with_sides(a_ref, low_ref, high_ref, row, p)
                buf[row, p] = v * spread(inv_ref, row, p, upper)
        part = pl.ds(start, stop - start)
        copies.append(pltpu.make_async_copy(buf.at[part], out_hbm.at[part], sem.at[e]))
        copies[-1].start()
    for copy in copies:
        copy.wait()


def last_ends(held, fb, fa, rb, ra, inv_ref, out_hbm, buf, sem):
    rows, pairs = out_hbm.shape[:2]
    upper = upper_half()
    face_odd = odd("face")
    for p in range(pairs):
        total_a, total_b = fa[p] + ra[p], fb[p] + rb[p]
        buf[0, p] = jnp.where(face_odd, total_a, total_b) * spread(inv_ref, 0, p, upper)
        buf[1, p] = jnp.where(face_odd, total_b, total_a) * spread(inv_ref, rows - 1, p, upper)
    copies = [
        pltpu.make_async_copy(buf.at[k], out_hbm.at[row], sem.at[k])
        for k, row in enumerate((0, rows - 1))
    ]
    for copy in copies:
        copy.start()
    for copy in copies:
        copy.wait()


def exchange(slot_a, slot_b, axis):
    n = lax.axis_size(axis)
    pairs_a = [(i, i ^ 1) for i in range(n)]
    pairs_b = [(i, (i + 1) % n if i % 2 else (i - 1) % n) for i in range(n)]
    got_b = lax.ppermute(slot_b, axis, pairs_b)
    got_a = lax.ppermute(slot_a, axis, pairs_a)
    return got_a, got_b


def call(kernel, outs, cost, args, scratch=(), far_in=0, far_out=False, alias=None):
    far = pl.BlockSpec(memory_space=pltpu.HBM)
    return pl.pallas_call(
        kernel,
        out_shape=[jax.ShapeDtypeStruct(s, F32) for s in outs],
        in_specs=[far] * far_in + [pl.BlockSpec()] * (len(args) - far_in),
        out_specs=[far if far_out else pl.BlockSpec()] * len(outs),
        scratch_shapes=scratch,
        input_output_aliases=alias or {},
        cost_estimate=pl.CostEstimate(flops=cost, bytes_accessed=cost // 4, transcendentals=0),
        compiler_params=pltpu.CompilerParams(vmem_limit_bytes=VMEM_LIMIT),
    )(*args)


def shards(fields, metric_diag, metric_cross, point_mass):
    nfield, rows, cols, nlev = fields.shape
    pairs, bands = cols // 2, rows // 4
    u = fields.transpose(1, 2, 0, 3).reshape(rows, pairs, 2 * nfield, nlev)
    md = metric_diag.transpose(1, 0, 2)
    full = (rows, pairs, 8, 128)
    edge = (pairs, 8, 128)
    heavy = (pairs + 1, 8, 128)
    side = (rows, 8, 128)
    line = (rows, 128)
    tall = ((rows + 7) // 8 * 8, 128)
    flops = 60 * rows * pairs * 8 * 128

    ends, ca, cb, s0, s1, sx, sm, uv = call(
        first_edges,
        [(rows, 4, 8, 128)] + [(rows + bands, 4, 128)] * 2 + [line] * 4 + [full],
        flops * 2 // 5,
        [pltpu.with_memory_space_constraint(x, pltpu.HBM)
         for x in (u, md, metric_cross, point_mass)],
        [VMEM(md.shape, F32), VMEM((rows, cols), F32), VMEM((rows, cols), F32),
         pltpu.SemaphoreType.DMA((bands + 3,))],
        far_in=4,
    )
    ga, gb = exchange(ca, cb, "col")
    a1, rf, rl = call(first_middle, [full, edge, edge], flops * 3 // 5, [uv, ends, s0, s1, sx])
    fb, fa, low, high, mcol = call(
        row_slots_mass, [heavy, heavy, side, side, line], flops // 50,
        [rf, rl, gb, ga, sm], [VMEM(tall, F32)] * 3,
    )
    ra, rb = exchange(fa, fb, "face")
    mid, invm = call(
        second_middle, [(rows - 8, pairs, 8, 128), line], flops * 3 // 5,
        [a1, low, high, mcol, s0, s1, sx],
    )
    a2, rf, rl, ca, cb, inv = call(
        second_ends, [full, edge, edge, (rows, 4, 128), (rows, 4, 128), line], flops * 2 // 5,
        [a1, mid, low, high, fb, fa, rb, ra, invm, s0, s1, sx], [VMEM(heavy, F32)] * 2,
    )
    ga, gb = exchange(ca, cb, "col")
    fb, fa, low, high = call(
        row_slots, [edge, edge, side, side], flops // 50, [rf, rl, gb, ga]
    )
    ra, rb = exchange(fa, fb, "face")
    (out,) = call(
        last_middle, [full], flops // 5, [a2, low, high, inv],
        [VMEM(full, F32), pltpu.SemaphoreType.DMA((bands,))], far_out=True,
    )
    (out,) = call(
        last_ends, [full], flops // 50, [out, fb, fa, rb, ra, inv],
        [VMEM((2,) + edge, F32), pltpu.SemaphoreType.DMA((2,))],
        far_in=1, far_out=True, alias={0: 0},
    )
    return out.reshape(rows, cols, nfield, nlev).transpose(2, 0, 1, 3)


def solution(mesh):
    return jax.shard_map(
        shards,
        mesh=mesh,
        in_specs=(
            P(None, "face", "col", None),
            P(None, "face", "col"),
            P("face", "col"),
            P("face", "col"),
        ),
        out_specs=P(None, "face", "col", None),
        check_vma=False,
    )
```

```python
import jax
import jax.numpy as jnp
import numpy as np
from jax import lax
from jax.experimental import pallas as pl
from jax.experimental.pallas import tpu as pltpu
from jax.sharding import PartitionSpec as P

F32 = jnp.float32
VMEM = pltpu.VMEM
VMEM_LIMIT = 6 * 2**20


def derivative_table():
    small = 1.0 / np.sqrt(5.0)
    nodes = np.array([-1.0, -small, small, 1.0])
    count = nodes.shape[0]
    weights = np.array(
        [np.prod([nodes[a] - nodes[k] for k in range(count) if k != a]) for a in range(count)]
    )
    table = np.zeros((count, count))
    for a in range(count):
        for b in range(count):
            if a == b:
                table[a, b] = np.sum([1.0 / (nodes[a] - nodes[k]) for k in range(count) if k != a])
            else:
                table[a, b] = weights[a] / weights[b] / (nodes[a] - nodes[b])
    return table.astype(np.float32)


D = derivative_table()


def upper_half():
    return lax.broadcasted_iota(jnp.int32, (8, 128), 0) >= 4


def swap(v):
    return pltpu.roll(v, 4, 0)


def col_coefs(table, upper):
    def vec(low, high):
        return jnp.where(upper, float(high), float(low)).astype(F32)

    return [
        [
            (vec(table[2 * h, 2 * k], table[2 * h + 1, 2 * k + 1]),
             vec(table[2 * h, 2 * k + 1], table[2 * h + 1, 2 * k]))
            for k in range(2)
        ]
        for h in range(2)
    ]


def col_apply(coefs, pair):
    swapped = [swap(v) for v in pair]
    out = []
    for h in range(2):
        (s0, x0), (s1, x1) = coefs[h]
        out.append((s0 * pair[0] + x0 * swapped[0]) + (s1 * pair[1] + x1 * swapped[1]))
    return out


def row_apply(table, vs):
    out = []
    for a in range(4):
        terms = [float(table[a, b]) * vs[b] for b in range(4)]
        out.append((terms[0] + terms[1]) + (terms[2] + terms[3]))
    return out


def spread(ref, row, pair, upper):
    line = jnp.broadcast_to(ref[pl.ds(row, 1), :], (8, 128))
    index = jnp.where(upper, 2 * pair + 1, 2 * pair).astype(jnp.int32)
    return jnp.take_along_axis(line, index, axis=1, mode="promise_in_bounds")


def element(load, base, g, mets, upper, fwd, bwd):
    d0, d1, dx = mets
    u = [[load(base + a, a, 2 * g + h) for h in range(2)] for a in range(4)]
    gx = [row_apply(D, [u[b][h] for b in range(4)]) for h in range(2)]
    fx = [[None] * 2 for _ in range(4)]
    wy = [None] * 4
    for a in range(4):
        gy = col_apply(fwd, u[a])
        fy = [None] * 2
        for h in range(2):
            p = 2 * g + h
            cross = spread(dx, base + a, p, upper)
            fx[a][h] = spread(d0, base + a, p, upper) * gx[h][a] + cross * gy[h]
            fy[h] = cross * gx[h][a] + spread(d1, base + a, p, upper) * gy[h]
        wy[a] = col_apply(bwd, fy)
    done = [[None] * 2 for _ in range(4)]
    for h in range(2):
        wx = row_apply(-D.T, [fx[b][h] for b in range(4)])
        for a in range(4):
            done[a][h] = wx[a] + wy[a][h]
    return done


def laplace_band(made, base, put, pairs, upper):
    lower = jnp.logical_not(upper)
    previous = None
    for g in range(pairs // 2):
        done = made(g)
        if previous is not None:
            for a in range(4):
                left, right = previous[a], done[a][0]
                put(base + a, 2 * g - 1, left + jnp.where(upper, swap(right), 0.0))
                done[a][0] = right + jnp.where(lower, swap(left), 0.0)
        for a in range(4):
            put(base + a, 2 * g, done[a][0])
        previous = [done[a][1] for a in range(4)]
    for a in range(4):
        put(base + a, pairs - 1, previous[a])


def join_rows(ref, row, pairs):
    for p in range(pairs):
        total = ref[row - 1, p] + ref[row, p]
        ref[row - 1, p] = total
        ref[row, p] = total


def constants():
    upper = upper_half()
    return upper, col_coefs(D, upper), col_coefs(-D.T, upper)


def odd(axis):
    return lax.rem(lax.axis_index(axis), 2) == 1


def put_slots(is_odd, index, first, last, slot_a, slot_b):
    slot_a[index] = jnp.where(is_odd, first, last)
    slot_b[index] = jnp.where(is_odd, last, first)


def first_edges(
    u_hbm, md_hbm, mc_hbm, mass_hbm,
    edge_ref, ca_ref, cb_ref, s0, s1, sx, sm, u_ref, md_v, mc_v, mass_v, sem,
):
    rows, pairs = u_hbm.shape[:2]
    cols = 2 * pairs
    bands = rows // 4

    def chunk(e, k):
        part = pl.ds(4 * e, 4)
        return pltpu.make_async_copy(
            u_hbm.at[part, pl.ds((pairs - 2) * k, 2)],
            u_ref.at[part, pl.ds(2 * k, 2)],
            sem.at[bands * k + e],
        )

    small = [
        pltpu.make_async_copy(source, dest, sem.at[2 * bands + k])
        for k, (source, dest) in enumerate(
            ((md_hbm, md_v), (mc_hbm, mc_v), (mass_hbm, mass_v))
        )
    ]
    for copy in small:
        copy.start()
    for e in range(bands):
        chunk(e, 0).start()
        chunk(e, 1).start()
    for copy in small:
        copy.wait()
    s0[:, 0:cols] = md_v[:, 0, :]
    s1[:, 0:cols] = md_v[:, 1, :]
    sx[:, 0:cols] = mc_v[...]
    sm[...] = jnp.ones_like(sm)
    sm[:, 0:cols] = mass_v[...]
    upper, fwd, bwd = constants()

    def band(e, carry):
        chunk(e, 0).wait()
        chunk(e, 1).wait()
        for k, g in enumerate((0, pairs // 2 - 1)):
            done = element(
                lambda row, a, p: u_ref[row, p - 2 * g + 2 * k], 4 * e, g, (s0, s1, sx), upper, fwd, bwd
            )
            for a in range(4):
                for h in range(2):
                    edge_ref[4 * e + a, 2 * k + h] = done[a][h]
        return carry

    lax.fori_loop(0, bands, band, 0)
    is_odd = odd("col")
    firsts = [edge_ref[r, 0] for r in range(rows)]
    lasts = [edge_ref[r, 3] for r in range(rows)]
    for r in range(rows):
        f, l = firsts[r], lasts[r]
        other = r - 1 if r % 4 == 0 else r + 1 if r % 4 == 3 else -1
        if 0 <= other < rows:
            f, l = f + firsts[other], l + lasts[other]
        put_slots(is_odd, r, f[0:4], l[4:8], ca_ref, cb_ref)
    for q in range(bands):
        part = sm[pl.ds(4 * q, 4), :]
        ca_ref[rows + q] = part
        cb_ref[rows + q] = part


def first_middle(u_hbm, edge_ref, s0, s1, sx, out_ref, rowf_ref, rowl_ref, u_ref, sem):
    rows, pairs = u_hbm.shape[:2]

    def chunk(e):
        part = pl.ds(4 * e, 4)
        return pltpu.make_async_copy(
            u_hbm.at[part, pl.ds(2, pairs - 4)], u_ref.at[part], sem.at[e]
        )

    for e in range(rows // 4):
        chunk(e).start()
    last = pairs // 2 - 1
    upper, fwd, bwd = constants()

    def band(e, carry):
        base = 4 * e
        chunk(e).wait()

        def made(g):
            if g in (0, last):
                k = 0 if g == 0 else 2
                return [[edge_ref[base + a, k + h] for h in range(2)] for a in range(4)]
            return element(
                lambda row, a, p: u_ref[row, p - 2], base, g, (s0, s1, sx), upper, fwd, bwd
            )

        def put(row, p, v):
            out_ref[row, p] = v

        laplace_band(made, base, put, pairs, upper)

        @pl.when(e > 0)
        def _():
            join_rows(out_ref, base, pairs)

        return carry

    lax.fori_loop(0, rows // 4, band, 0)
    for p in range(pairs):
        rowf_ref[p] = out_ref[0, p]
        rowl_ref[p] = out_ref[rows - 1, p]


def row_slots(rowf, rowl, rb, ra, fb_ref, fa_ref, low_ref, high_ref):
    pairs, rows = rowf.shape[0], low_ref.shape[0]
    col_odd, face_odd = odd("col"), odd("face")
    zero = jnp.zeros((4, 128), F32)
    for r in range(rows):
        a, b = ra[r], rb[r]
        low = jnp.concatenate([jnp.where(col_odd, a, b), zero], axis=0)
        high = jnp.concatenate([zero, jnp.where(col_odd, b, a)], axis=0)
        low_ref[r] = low
        high_ref[r] = high
    for p in range(pairs):
        f, l = rowf[p], rowl[p]
        if p == 0:
            f, l = f + low_ref[0], l + low_ref[rows - 1]
        if p == pairs - 1:
            f, l = f + high_ref[0], l + high_ref[rows - 1]
        put_slots(face_odd, p, f, l, fa_ref, fb_ref)


def row_slots_mass(
    rowf, rowl, rb, ra, mass, fb_ref, fa_ref, low_ref, high_ref, mcol_ref, sb, sa, sm,
):
    pairs, rows = rowf.shape[0], mass.shape[0]
    cols = 2 * pairs
    row_slots(rowf, rowl, rb, ra, fb_ref, fa_ref, low_ref, high_ref)
    col_odd = odd("col")
    for q in range(rows // 4):
        part = pl.ds(4 * q, 4)
        a, b = ra[rows + q], rb[rows + q]
        sb[part, :] = jnp.where(col_odd, a, b)
        sa[part, :] = jnp.where(col_odd, b, a)
    sm[...] = jnp.ones_like(sm)
    sm[pl.ds(0, rows), :] = mass[...]
    m = sm[...]
    lane = lax.broadcasted_iota(jnp.int32, m.shape, 1)
    prev = jnp.where(lane == 0, pltpu.roll(sb[...], 128 - (cols - 1), 1), pltpu.roll(m, 1, 1))
    following = jnp.where(
        lane == cols - 1, pltpu.roll(sa[...], cols - 1, 1), pltpu.roll(m, 127, 1)
    )
    m = m + jnp.where(lane % 4 == 0, prev, 0.0) + jnp.where(lane % 4 == 3, following, 0.0)
    sm[...] = m
    mcol_ref[...] = sm[pl.ds(0, rows), :]
    first = jnp.broadcast_to(sm[pl.ds(0, 1), :], (8, 128))
    final = jnp.broadcast_to(sm[pl.ds(rows - 1, 1), :], (8, 128))
    put_slots(odd("face"), pairs, first, final, fa_ref, fb_ref)


def with_sides(a_ref, low_ref, high_ref, row, p):
    v = a_ref[row, p]
    if p == 0:
        v = v + low_ref[row]
    if p == a_ref.shape[1] - 1:
        v = v + high_ref[row]
    return v


def second_middle(a_ref, low_ref, high_ref, mcol_ref, s0, s1, sx, out_ref, inv_ref):
    rows, pairs = a_ref.shape[:2]
    bands = rows // 4
    upper, fwd, bwd = constants()
    inv_ref[pl.ds(0, 1), :] = mcol_ref[pl.ds(0, 1), :]
    inv_ref[pl.ds(rows - 1, 1), :] = mcol_ref[pl.ds(rows - 1, 1), :]
    for e in range(bands):
        inv_ref[pl.ds(4 * e + 1, 2), :] = 1.0 / mcol_ref[pl.ds(4 * e + 1, 2), :]
        if e > 0:
            total = 1.0 / (mcol_ref[pl.ds(4 * e - 1, 1), :] + mcol_ref[pl.ds(4 * e, 1), :])
            inv_ref[pl.ds(4 * e - 1, 1), :] = total
            inv_ref[pl.ds(4 * e, 1), :] = total

    def band(e, carry):
        base = 4 * e

        def load(row, a, p):
            v = with_sides(a_ref, low_ref, high_ref, row, p)
            return v * spread(inv_ref, row, p, upper)

        def put(row, p, v):
            out_ref[row - 4, p] = v

        laplace_band(
            lambda g: element(load, base, g, (s0, s1, sx), upper, fwd, bwd),
            base, put, pairs, upper,
        )

        @pl.when(e > 1)
        def _():
            join_rows(out_ref, base - 4, pairs)

        return carry

    lax.fori_loop(1, bands - 1, band, 0)


def second_ends(
    a_ref, mid_ref, low_ref, high_ref, fb, fa, rb, ra, invm_ref, s0, s1, sx,
    out_ref, rowf_ref, rowl_ref, ca_ref, cb_ref, inv_ref, tf, tl,
):
    rows, pairs = a_ref.shape[:2]
    last = rows // 4 - 1
    upper, fwd, bwd = constants()
    face_odd = odd("face")
    for p in range(pairs + 1):
        total_a, total_b = fa[p] + ra[p], fb[p] + rb[p]
        tf[p] = jnp.where(face_odd, total_a, total_b)
        tl[p] = jnp.where(face_odd, total_b, total_a)
    inv_ref[...] = invm_ref[...]
    inv_ref[pl.ds(0, 1), :] = 1.0 / tf[pairs, 0:1]
    inv_ref[pl.ds(rows - 1, 1), :] = 1.0 / tl[pairs, 0:1]

    def band(k, carry):
        base = 4 * last * k

        def load(row, a, p):
            v = with_sides(a_ref, low_ref, high_ref, row, p)
            if a == 0:
                v = jnp.where(k == 0, tf[p], v)
            if a == 3:
                v = jnp.where(k == 1, tl[p], v)
            return v * spread(inv_ref, row, p, upper)

        def put(row, p, v):
            out_ref[row, p] = v

        laplace_band(
            lambda g: element(load, base, g, (s0, s1, sx), upper, fwd, bwd),
            base, put, pairs, upper,
        )
        return carry

    lax.fori_loop(0, 2, band, 0)

    def carry_over(r, carry):
        for p in range(pairs):
            out_ref[r, p] = mid_ref[r - 4, p]
        return carry

    lax.fori_loop(4, rows - 4, carry_over, 0)
    join_rows(out_ref, 4, pairs)
    join_rows(out_ref, rows - 4, pairs)
    for p in range(pairs):
        rowf_ref[p] = out_ref[0, p]
        rowl_ref[p] = out_ref[rows - 1, p]
    is_odd = odd("col")
    for r in range(rows):
        put_slots(is_odd, r, out_ref[r, 0][0:4], out_ref[r, pairs - 1][4:8], ca_ref, cb_ref)


def last_middle(a_ref, low_ref, high_ref, inv_ref, out_hbm, buf, sem):
    rows, pairs = a_ref.shape[:2]
    bands = rows // 4
    upper = upper_half()
    copies = []
    for e in range(bands):
        start = 1 if e == 0 else 4 * e
        stop = rows - 1 if e == bands - 1 else 4 * e + 4
        for row in range(start, stop):
            for p in range(pairs):
                v = with_sides(a_ref, low_ref, high_ref, row, p)
                buf[row, p] = v * spread(inv_ref, row, p, upper)
        part = pl.ds(start, stop - start)
        copies.append(pltpu.make_async_copy(buf.at[part], out_hbm.at[part], sem.at[e]))
        copies[-1].start()
    for copy in copies:
        copy.wait()


def last_ends(held, fb, fa, rb, ra, inv_ref, out_hbm, buf, sem):
    rows, pairs = out_hbm.shape[:2]
    upper = upper_half()
    face_odd = odd("face")
    for p in range(pairs):
        total_a, total_b = fa[p] + ra[p], fb[p] + rb[p]
        buf[0, p] = jnp.where(face_odd, total_a, total_b) * spread(inv_ref, 0, p, upper)
        buf[1, p] = jnp.where(face_odd, total_b, total_a) * spread(inv_ref, rows - 1, p, upper)
    copies = [
        pltpu.make_async_copy(buf.at[k], out_hbm.at[row], sem.at[k])
        for k, row in enumerate((0, rows - 1))
    ]
    for copy in copies:
        copy.start()
    for copy in copies:
        copy.wait()


def exchange(slot_a, slot_b, axis):
    n = lax.axis_size(axis)
    pairs_a = [(i, i ^ 1) for i in range(n)]
    pairs_b = [(i, (i + 1) % n if i % 2 else (i - 1) % n) for i in range(n)]
    got_b = lax.ppermute(slot_b, axis, pairs_b)
    got_a = lax.ppermute(slot_a, axis, pairs_a)
    return got_a, got_b


def call(kernel, outs, cost, args, scratch=(), far_in=0, far_out=False, alias=None):
    far = pl.BlockSpec(memory_space=pltpu.HBM)
    return pl.pallas_call(
        kernel,
        out_shape=[jax.ShapeDtypeStruct(s, F32) for s in outs],
        in_specs=[far] * far_in + [pl.BlockSpec()] * (len(args) - far_in),
        out_specs=[far if far_out else pl.BlockSpec()] * len(outs),
        scratch_shapes=scratch,
        input_output_aliases=alias or {},
        cost_estimate=pl.CostEstimate(flops=cost, bytes_accessed=cost // 4, transcendentals=0),
        compiler_params=pltpu.CompilerParams(vmem_limit_bytes=VMEM_LIMIT),
    )(*args)


def shards(fields, metric_diag, metric_cross, point_mass):
    nfield, rows, cols, nlev = fields.shape
    pairs, bands = cols // 2, rows // 4
    u = fields.transpose(1, 2, 0, 3).reshape(rows, pairs, 2 * nfield, nlev)
    md = metric_diag.transpose(1, 0, 2)
    full = (rows, pairs, 8, 128)
    edge = (pairs, 8, 128)
    heavy = (pairs + 1, 8, 128)
    side = (rows, 8, 128)
    line = (rows, 128)
    tall = ((rows + 7) // 8 * 8, 128)
    flops = 60 * rows * pairs * 8 * 128

    u, *rest = (
        pltpu.with_memory_space_constraint(x, pltpu.HBM)
        for x in (u, md, metric_cross, point_mass)
    )
    ends, ca, cb, s0, s1, sx, sm = call(
        first_edges,
        [(rows, 4, 8, 128)] + [(rows + bands, 4, 128)] * 2 + [line] * 4,
        flops * 2 // 5,
        [u, *rest],
        [VMEM((rows, 4, 8, 128), F32), VMEM(md.shape, F32), VMEM((rows, cols), F32), VMEM((rows, cols), F32),
         pltpu.SemaphoreType.DMA((2 * bands + 3,))],
        far_in=4,
    )
    ga, gb = exchange(ca, cb, "col")
    a1, rf, rl = call(first_middle, [full, edge, edge], flops * 3 // 5, [u, ends, s0, s1, sx],
        [VMEM((rows, pairs - 4, 8, 128), F32), pltpu.SemaphoreType.DMA((bands,))], far_in=1,
    )
    fb, fa, low, high, mcol = call(
        row_slots_mass, [heavy, heavy, side, side, line], flops // 50,
        [rf, rl, gb, ga, sm], [VMEM(tall, F32)] * 3,
    )
    ra, rb = exchange(fa, fb, "face")
    mid, invm = call(
        second_middle, [(rows - 8, pairs, 8, 128), line], flops * 3 // 5,
        [a1, low, high, mcol, s0, s1, sx],
    )
    a2, rf, rl, ca, cb, inv = call(
        second_ends, [full, edge, edge, (rows, 4, 128), (rows, 4, 128), line], flops * 2 // 5,
        [a1, mid, low, high, fb, fa, rb, ra, invm, s0, s1, sx], [VMEM(heavy, F32)] * 2,
    )
    ga, gb = exchange(ca, cb, "col")
    fb, fa, low, high = call(
        row_slots, [edge, edge, side, side], flops // 50, [rf, rl, gb, ga]
    )
    ra, rb = exchange(fa, fb, "face")
    (out,) = call(
        last_middle, [full], flops // 5, [a2, low, high, inv],
        [VMEM(full, F32), pltpu.SemaphoreType.DMA((bands,))], far_out=True,
    )
    (out,) = call(
        last_ends, [full], flops // 50, [out, fb, fa, rb, ra, inv],
        [VMEM((2,) + edge, F32), pltpu.SemaphoreType.DMA((2,))],
        far_in=1, far_out=True, alias={0: 0},
    )
    return out.reshape(rows, cols, nfield, nlev).transpose(2, 0, 1, 3)


def solution(mesh):
    return jax.shard_map(
        shards,
        mesh=mesh,
        in_specs=(
            P(None, "face", "col", None),
            P(None, "face", "col"),
            P("face", "col"),
            P("face", "col"),
        ),
        out_specs=P(None, "face", "col", None),
        check_vma=False,
    )
```
